32 devices in a mesh: tm: 16 (over z, y, x), space: 2 (over core).
Axes of the slice: x: 2, y: 2, z: 4, core: 2. Of those that a mesh axis runs over, the one named last changes fastest.
Arguments:
- forcing: float32 [16, 64, 64, 256], P('tm', None, None, 'space'), may hold values from -6 to 6
- initial: float32 [64, 64, 256], P('tm', None, 'space'), may hold values from -6 to 6
- diffusion: float32 [64, 64, 256], P('tm', None, 'space'), may hold values from 0.25 to 4
- drift: float32 [64, 64, 256], P('tm', None, 'space'), may hold values from 0.2 to 1.5
Outputs:
- states: float32 [16, 64, 64, 256], P('tm', None, None, 'space')
The draws below stay inside these ranges and needn't reach their ends.
All inputs are finite; a program needn't handle non-finite values.
Results may differ from the reference program's by a relative error of at most 0.00002.
Values sent between devices are 32-bit elements; how exact they have to be, the bound alone decides.
No kernel may reach another device: no remote copies, remote signals or barrier semaphores. Data moves between devices by JAX's collectives and lax.ppermute only.
A program may use at most 64 MiB of HBM per device.

```python
import math
import jax
import jax.numpy as jnp
from jax import lax

NT = 16
NX = 64
SWEEPS = 4
XS = 1
NZ = 64
NY = 256


def steps_of(own_key, dims, cuts, smallest, high):
    loudness = 1.0
    for position, blocks in cuts:
        steps = jax.random.uniform(jax.random.fold_in(jax.random.fold_in(own_key, 6), position), (blocks,), jnp.float32, smallest / len(cuts), high / len(cuts))
        loudness = loudness * jnp.repeat(jnp.exp(steps), dims[position] // blocks).reshape((-1,) + (1,) * (len(dims) - 1 - position))
    return loudness


def noise(own_key, shape, spread, reach, pieces=(), dtype=jnp.bfloat16):
    loudness = steps_of(own_key, shape, pieces, -0.22, 0.18) if pieces else 1.0
    drawn = jax.random.normal(own_key, shape, jnp.float32) * spread * loudness
    return jnp.minimum(jnp.maximum(drawn, -reach), reach).astype(dtype)


def setup_inputs(seed: int = 0) -> dict:
    arg_keys = jax.random.split(jax.random.key(seed), 5)
    return {
        "forcing": noise(arg_keys[0], (NT * XS, NZ, NX // XS, NY), 1.0, 6.0, ((0, 16), (3, 2)), jnp.float32),
        "initial": noise(arg_keys[1], (NZ, NX, NY), 1.0, 6.0, ((0, 16), (2, 2)), jnp.float32),
        "diffusion": jnp.clip(jnp.exp(math.log(4.0) - 2.7725887 * jax.random.uniform(arg_keys[2], (NZ, NX, NY), jnp.float32) ** steps_of(arg_keys[2], (NZ, NX, NY), ((0, 16), (2, 2)), -0.2, 0.2)), 0.25, 4.0),
        "drift": jnp.clip(0.2 + 1.3 * jax.random.uniform(arg_keys[3], (NZ, NX, NY), jnp.float32) ** steps_of(arg_keys[3], (NZ, NX, NY), ((0, 16), (2, 2)), -0.2, 0.2), 0.2, 1.5),
    }


def relax_cells(field, source, diffus, drift_rate):
    widened = jnp.pad(field, ((0, 0), (1, 1), (0, 0)))
    beside = field[2:, :, 1:-1] + field[:-2, :, 1:-1]
    beside = beside + field[1:-1, :, 2:] + field[1:-1, :, :-2]
    beside = beside + widened[1:-1, 2:, 1:-1] + widened[1:-1, :-2, 1:-1]
    upstream = field[:-2, :, 1:-1]
    return (source + diffus * beside + drift_rate * upstream) / (1.0 + 6.0 * diffus + drift_rate)


def reference(forcing, initial, diffusion, drift):
    nzall = forcing.shape[1]
    xpart = forcing.shape[2]
    nyall = forcing.shape[3]
    force = forcing.reshape(NT, XS, nzall, xpart, nyall).transpose(0, 2, 1, 3, 4)
    force = force.reshape(NT, nzall, XS * xpart, nyall)

    def advance(current, forcing_now):
        source = current + forcing_now
        field = current
        for sweep_index in range(SWEEPS):
            padded = jnp.pad(field, ((1, 1), (0, 0), (1, 1)))
            field = relax_cells(padded, source, diffusion, drift)
        return field, field

    final, result = lax.scan(advance, initial, force)
    result = result.reshape(NT, nzall, XS, xpart, nyall).transpose(0, 2, 1, 3, 4)
    return result.reshape(NT * XS, nzall, xpart, nyall)
```

```python
import functools

import jax
import jax.numpy as jnp
from jax import lax
from jax.experimental import pallas as pl
from jax.experimental.pallas import tpu as pltpu
from jax.sharding import PartitionSpec as P

NT = 16
SWEEPS = 4
LANES = 128
ROWS = 8


def padded(shard, sides, width):
    for axis, dim in sides:
        size, length = (lax.axis_size(axis), shard.shape[dim])
        up = [(i, (i + 1) % size) for i in range(size - 1)]
        down = [(j, i) for i, j in up]
        last = lax.slice_in_dim(shard, length - width, length, axis=dim)
        leading = lax.slice_in_dim(shard, 0, width, axis=dim)
        before = lax.ppermute(last, axis, up)
        after = lax.ppermute(leading, axis, down)
        shard = jnp.concatenate([before, shard, after], axis=dim)
    return shard


def relax_cells(field, source, diffus, drift_rate):
    widened = jnp.pad(field, ((0, 0), (1, 1), (0, 0)))
    beside = field[2:, :, 1:-1] + field[:-2, :, 1:-1]
    beside = beside + field[1:-1, :, 2:] + field[1:-1, :, :-2]
    beside = beside + widened[1:-1, 2:, 1:-1] + widened[1:-1, :-2, 1:-1]
    upstream = field[:-2, :, 1:-1]
    return (source + diffus * beside + drift_rate * upstream) / (1.0 + 6.0 * diffus + drift_rate)


def trim_rim(values, margin_cut):
    zlen = values.shape[-3]
    ylen = values.shape[-1]
    return values[..., margin_cut : zlen - margin_cut, :, margin_cut : ylen - margin_cut]


def sweep_block(widened, coef_wide, depth):
    grown = widened[0]
    for inner in range(depth):
        margin_cut = inner + 1
        grown = relax_cells(
            grown,
            trim_rim(widened[1], margin_cut),
            trim_rim(coef_wide[0], margin_cut),
            trim_rim(coef_wide[1], margin_cut),
        )
    return grown


def split_along_z(forcing, initial, diffusion, drift):
    xparts = lax.axis_size("tm") // NT
    slabs = lax.all_to_all(forcing, "tm", split_axis=1, concat_axis=0, tiled=True)
    zcells = slabs.shape[1]
    xpart = slabs.shape[2]
    ycells = slabs.shape[3]
    slabs = slabs.reshape(NT, xparts, zcells, xpart, ycells).transpose(0, 2, 1, 3, 4)
    slabs = slabs.reshape(NT, zcells, xparts * xpart, ycells)
    coeffs = jnp.stack((diffusion, drift))
    coef_wide = padded(coeffs, (("tm", 1), ("space", 3)), SWEEPS)

    def advance(current, forcing_now):
        source = current + forcing_now
        field = current
        widened = padded(jnp.stack((field, source)), (("tm", 1), ("space", 3)), SWEEPS)
        field = sweep_block(widened, coef_wide, SWEEPS)
        return (field, field)

    final, result = lax.scan(advance, initial, slabs)
    result = result.reshape(NT, zcells, xparts, xpart, ycells).transpose(0, 2, 1, 3, 4)
    result = result.reshape(NT * xparts, zcells, xpart, ycells)
    return lax.all_to_all(result, "tm", split_axis=0, concat_axis=1, tiled=True)


def gray(i):
    return i ^ (i >> 1)


def call(kernel, out_shape, operands, flags, scratch=(), flops=0, name=None):
    size = sum(x.size * x.dtype.itemsize for x in operands)
    shapes = out_shape if isinstance(out_shape, (tuple, list)) else (out_shape,)
    size += sum(functools.reduce(lambda a, b: a * b, x.shape) * 4 for x in shapes)
    return pl.pallas_call(
        kernel,
        out_shape=out_shape,
        in_specs=[pl.BlockSpec(memory_space=pltpu.SMEM)]
        + [pl.BlockSpec(memory_space=pltpu.VMEM)] * len(operands),
        out_specs=jax.tree.map(lambda _: pl.BlockSpec(memory_space=pltpu.VMEM), out_shape),
        scratch_shapes=list(scratch),
        cost_estimate=pl.CostEstimate(flops=flops or size, bytes_accessed=size, transcendentals=0),
        name=name,
    )(flags, *operands)


def left_lanes():
    return lax.broadcasted_iota(jnp.int32, (ROWS, LANES), 1) < LANES // 2


def swap_lanes(v):
    return pltpu.roll(v, LANES // 2, 1)


def format_kernel(blocks, flags, raw, keep, send):
    zrows = raw.shape[0]
    left = left_lanes()

    def body(core):
        def step(pair, carry):
            both = raw[pl.ds(2 * pair, 2)].reshape(LANES, LANES).T
            for r in range(blocks):
                low = both[2 * ROWS * r : 2 * ROWS * r + ROWS]
                high = both[2 * ROWS * r + ROWS : 2 * ROWS * (r + 1)]
                first = jnp.where(left, low, swap_lanes(high))
                second = jnp.where(left, swap_lanes(low), high)
                slot = gray(core * (blocks // 2) + r // 2) % (blocks // 2)
                to = keep if gray(r) & 1 == core else send
                start = slot * ROWS * zrows + 2 * pair
                to[pl.ds(start, ROWS, stride=zrows), :] = first
                to[pl.ds(start + 1, ROWS, stride=zrows), :] = second
            return carry

        lax.fori_loop(0, zrows // 2, step, 0)

    for core in range(2):
        pl.when(flags[1] == core)(functools.partial(body, core))


def unformat_kernel(blocks, flags, keep, got, out):
    zrows = out.shape[0]
    left = left_lanes()

    def body(core):
        def step(pair, carry):
            columns = []
            for r in range(blocks):
                slot = gray(core * (blocks // 2) + r // 2) % (blocks // 2)
                src = keep if gray(r) & 1 == core else got
                start = slot * ROWS * zrows + 2 * pair
                first = src[pl.ds(start, ROWS, stride=zrows), :]
                second = src[pl.ds(start + 1, ROWS, stride=zrows), :]
                columns.append(jnp.where(left, first, swap_lanes(second)))
                columns.append(jnp.where(left, swap_lanes(first), second))
            both = jnp.concatenate(columns, axis=0).T
            out[pl.ds(2 * pair, 2)] = both.reshape(2, LANES // 2, LANES)
            return carry

        lax.fori_loop(0, zrows // 2, step, 0)

    for core in range(2):
        pl.when(flags[1] == core)(functools.partial(body, core))


def arrange_kernel(zpart, flags, got, out):
    chips, arrays = got.shape[0], out.shape[0]
    for k in range(arrays):
        for chip in range(chips):
            for upper in range(2):
                rows = pl.ds((2 * k + upper) * zpart, zpart)
                z = (upper * chips + chip) * zpart
                out[k, :, pl.ds(z, zpart), :] = got[chip, :, rows, :]


class Region:
    def __init__(self, even):
        self.even = even
        left = left_lanes()[None]
        self.left = left
        self.other = jnp.logical_xor(left, jnp.full((1, ROWS, LANES), even, jnp.int32) == 1)

    def tiles(self, plane):
        return plane.reshape(-1, ROWS, LANES)

    def plane(self, kind, m, own, core, link):
        back = ROWS - 1 - m
        if kind == "own":
            v = jnp.where(self.left, self.tiles(own[m]), self.tiles(own[back]))
        elif kind == "far":
            c = self.tiles(core[jnp.where(self.even == 1, back, m)])
            n = self.tiles(link[jnp.where(self.even == 1, m, back)])
            v = jnp.where(self.other, c, n)
        else:
            c = self.tiles(core[jnp.where(self.even == 1, m, back)])
            n = self.tiles(link[jnp.where(self.even == 1, back, m)])
            v = pltpu.roll(jnp.where(self.other, n, c), LANES // 2, 2)
        return v.reshape(-1, LANES)

    def fill(self, first, own, core, link, put):
        def run(kind, lo, hi, place):
            def step(m, carry):
                put(place(m), self.plane(kind, m, own, core, link))
                return carry

            if lo < hi:
                lax.fori_loop(lo, hi, step, 0)

        run("far", first, ROWS, lambda m: m)
        run("near", 0, min(ROWS, 2 * ROWS - first), lambda m: 2 * ROWS - 1 - m)
        run("own", 0, ROWS, lambda m: 2 * ROWS + m)


def prep_kernel(flags, own, core, link, coef):
    region = Region(flags[0])

    def put_diffusion(i, d):
        coef[0, i] = d

    def put_drift(i, r):
        d = coef[0, i]
        inv = 1.0 / (1.0 + 6.0 * d + r)
        coef[0, i] = d * inv
        coef[1, i] = (d + r) * inv
        coef[2, i] = inv

    region.fill(0, own.at[1], core.at[1], link.at[1], put_diffusion)
    region.fill(0, own.at[2], core.at[2], link.at[2], put_drift)


def window_kernel(flags, own, core, link, f_own, f_core, f_link, coef, out, va, vb, c):
    steps, planes, zrows = out.shape[0], 3 * ROWS, own.shape[1]
    top = 2 * ROWS
    region = Region(flags[0])
    lane = lax.broadcasted_iota(jnp.int32, (ROWS, LANES), 1) % (LANES // 2)
    first_x, last_x = lane == 0, lane == LANES // 2 - 1
    inside = pl.ds(ROWS, zrows)
    for v in (va, vb):
        v[:, 0:ROWS] = jnp.zeros((planes + 1, ROWS, LANES), jnp.float32)
        v[:, zrows + ROWS :] = jnp.zeros((planes + 1, ROWS, LANES), jnp.float32)

    def put_field(i, plane):
        va[i, inside] = plane

    region.fill(0, own, core, link, put_field)
    va[planes, inside] = swap_lanes(va[planes - 1, inside])

    src, dst = va, vb
    for step in range(steps):
        current = src

        def put_source(i, plane):
            c[i] = coef[2, i] * (current[i, inside] + plane)

        region.fill(SWEEPS * step + 1, f_own.at[step], f_core.at[step], f_link.at[step], put_source)
        for sweep in range(SWEEPS):

            def relax(i, carry, src=src, dst=dst):
                for z in range(0, zrows, ROWS):
                    at = ROWS + z
                    v = src[i, at : at + ROWS]
                    zm = src[i, at - 1 : at + ROWS - 1]
                    total = src[i, at + 1 : at + ROWS + 1]
                    total += src[i - 1, at : at + ROWS] + src[i + 1, at : at + ROWS]
                    total += jnp.where(first_x, 0.0, pltpu.roll(v, 1, 1))
                    total += jnp.where(last_x, 0.0, pltpu.roll(v, LANES - 1, 1))
                    rows = slice(z, z + ROWS)
                    dst[i, at : at + ROWS] = c[i, rows] + coef[0, i, rows] * total + coef[1, i, rows] * zm
                return carry

            lax.fori_loop(SWEEPS * step + sweep + 1, planes, relax, 0)
            dst[planes, inside] = swap_lanes(dst[planes - 1, inside])
            src, dst = dst, src
        for m in range(ROWS):
            low = src[top + m, inside].reshape(-1, ROWS, LANES)
            high = src[planes - 1 - m, inside].reshape(-1, ROWS, LANES)
            out[step, m] = jnp.where(region.left, low, high).reshape(-1, LANES)


def split_along_y(forcing, initial, diffusion, drift):
    f32 = jnp.float32
    chips = lax.axis_size("tm") // 2
    zpart, xlen, ylen = initial.shape
    zlen = forcing.shape[1]
    blocks = ylen // (2 * ROWS)
    spw = 2 * ROWS // SWEEPS
    t, s = lax.axis_index("tm"), lax.axis_index("space")
    device = 2 * (t % chips) + s
    odd = device
    for shift in (1, 2, 4, 8):
        odd = odd ^ (odd >> shift)
    lower = t < chips
    flags = jnp.stack([1 - (odd & 1), s, jnp.int32(0)]).astype(jnp.int32)
    groups = [list(range(chips)), list(range(chips, 2 * chips))]
    both = ("tm", "space")
    across = []
    for b in range(1, 2 * chips - 1, 2):
        for base in (0, 2 * chips):
            i, j = base + gray(b), base + gray(b + 1)
            across += [(i, j), (j, i)]
    hop = [(i, 2 * chips + i) for i in range(2 * chips)]
    cores = [(0, 1), (1, 0)]

    def exchange(x):
        return lax.ppermute(x, "space", cores), lax.ppermute(x, both, across)

    def to_blocks(raw):
        zr = raw.shape[0]
        part = jax.ShapeDtypeStruct((blocks // 2 * ROWS * zr, LANES), f32)
        keep, send = call(
            functools.partial(format_kernel, blocks), (part, part), (raw,), flags, name="format"
        )
        got = lax.ppermute(send, "space", cores)
        whole = jnp.where(s == 0, jnp.concatenate([keep, got]), jnp.concatenate([got, keep]))
        whole = whole.reshape(chips, ROWS, zr, LANES)
        return lax.all_to_all(whole, "tm", 0, 0, axis_index_groups=groups, tiled=True)

    fields = jnp.stack((initial, diffusion, drift))
    far = lax.ppermute(fields, "tm", [(i, (i + chips) % (2 * chips)) for i in range(2 * chips)])
    low, high = jnp.where(lower, fields, far), jnp.where(lower, far, fields)
    fields = jnp.concatenate([low[:, None], high[:, None]], axis=1).reshape(-1, xlen, ylen)

    force = to_blocks(forcing.reshape(zlen, xlen, ylen))
    fields = to_blocks(fields)
    fields = call(
        functools.partial(arrange_kernel, zpart),
        jax.ShapeDtypeStruct((3, ROWS, zlen, LANES), f32),
        (fields,),
        flags,
        name="arrange",
    )
    near = exchange(fields)
    region = jax.ShapeDtypeStruct((3, 3 * ROWS, zlen, LANES), f32)
    coef = call(prep_kernel, region, (fields, *near), flags, name="prep")
    windows = []
    for k in range(0, chips, spw):
        part = force[k : k + spw]
        windows.append((part, *exchange(part)))

    wide = pltpu.VMEM((3 * ROWS + 1, zlen + 2 * ROWS, LANES), f32)
    scratch = (wide, wide, pltpu.VMEM((3 * ROWS, zlen, LANES), f32))
    sweeps = spw * SWEEPS
    flops = 10 * sweeps * 2 * ROWS * zlen * LANES

    def window(state, beside, part):
        return call(
            window_kernel,
            jax.ShapeDtypeStruct((spw, ROWS, zlen, LANES), f32),
            (state, *beside, *part, coef),
            flags,
            scratch,
            flops,
            name="window",
        )

    start = fields[0]
    state, beside = start, (near[0][0], near[1][0])
    for stage in range(2):
        outs = []
        for k, part in enumerate(windows):
            if k or stage:
                beside = exchange(state)
            outs.append(window(state, beside, part))
            state = outs[-1][-1]
        if stage == 0:
            state = jnp.where(lower, start, lax.ppermute(state, both, hop))

    result = jnp.concatenate(outs)
    result = lax.all_to_all(result, "tm", 0, 0, axis_index_groups=groups, tiled=True)
    half = chips // 2
    keep = lax.dynamic_slice_in_dim(result, s * half, half)
    send = lax.dynamic_slice_in_dim(result, (1 - s) * half, half)
    got = lax.ppermute(send, "space", cores)
    out = call(
        functools.partial(unformat_kernel, blocks),
        jax.ShapeDtypeStruct((zlen, xlen, ylen), f32),
        (keep.reshape(-1, LANES), got.reshape(-1, LANES)),
        flags,
        name="unformat",
    )
    return out[None]


def per_device(forcing, initial, diffusion, drift):
    tm, space = lax.axis_size("tm"), lax.axis_size("space")
    zpart, xlen, ylen = initial.shape
    chips, spw = tm // 2, 2 * ROWS // SWEEPS
    along_y = (
        tm == NT
        and space == 2
        and forcing.shape == (1, tm * zpart, xlen, ylen)
        and 2 * xlen == LANES
        and ylen == LANES
        and ylen * space == 2 * ROWS * 2 * chips
        and chips % spw == 0
        and chips * zpart % ROWS == 0
    )
    plan = split_along_y if along_y else split_along_z
    return plan(forcing, initial, diffusion, drift)


def solution(mesh):
    in_specs = (
        P("tm", None, None, "space"),
        P("tm", None, "space"),
        P("tm", None, "space"),
        P("tm", None, "space"),
    )
    out_specs = P("tm", None, None, "space")
    return jax.shard_map(
        per_device, mesh=mesh, in_specs=in_specs, out_specs=out_specs, check_vma=False
    )
```

```python
import functools
import math

import jax
import jax.numpy as jnp
from jax import lax
from jax.experimental import pallas as pl
from jax.experimental.pallas import tpu as pltpu
from jax.sharding import PartitionSpec as P


NT = 16
SWEEPS = 4
LANES = 128
ROWS = 8
FILL = 4
BATCH = 24


def padded(shard, sides, width):
    for axis, dim in sides:
        size, length = (lax.axis_size(axis), shard.shape[dim])
        up = [(i, (i + 1) % size) for i in range(size - 1)]
        down = [(j, i) for i, j in up]
        last = lax.slice_in_dim(shard, length - width, length, axis=dim)
        leading = lax.slice_in_dim(shard, 0, width, axis=dim)
        before = lax.ppermute(last, axis, up)
        after = lax.ppermute(leading, axis, down)
        shard = jnp.concatenate([before, shard, after], axis=dim)
    return shard


def relax_cells(field, source, diffus, drift_rate):
    widened = jnp.pad(field, ((0, 0), (1, 1), (0, 0)))
    beside = field[2:, :, 1:-1] + field[:-2, :, 1:-1]
    beside = beside + field[1:-1, :, 2:] + field[1:-1, :, :-2]
    beside = beside + widened[1:-1, 2:, 1:-1] + widened[1:-1, :-2, 1:-1]
    upstream = field[:-2, :, 1:-1]
    return (source + diffus * beside + drift_rate * upstream) / (1.0 + 6.0 * diffus + drift_rate)


def trim_rim(values, margin_cut):
    zlen = values.shape[-3]
    ylen = values.shape[-1]
    return values[..., margin_cut : zlen - margin_cut, :, margin_cut : ylen - margin_cut]


def sweep_block(widened, coef_wide, depth):
    grown = widened[0]
    for inner in range(depth):
        margin_cut = inner + 1
        grown = relax_cells(
            grown,
            trim_rim(widened[1], margin_cut),
            trim_rim(coef_wide[0], margin_cut),
            trim_rim(coef_wide[1], margin_cut),
        )
    return grown


def split_along_z(forcing, initial, diffusion, drift):
    xparts = lax.axis_size("tm") // NT
    slabs = lax.all_to_all(forcing, "tm", split_axis=1, concat_axis=0, tiled=True)
    zcells = slabs.shape[1]
    xpart = slabs.shape[2]
    ycells = slabs.shape[3]
    slabs = slabs.reshape(NT, xparts, zcells, xpart, ycells).transpose(0, 2, 1, 3, 4)
    slabs = slabs.reshape(NT, zcells, xparts * xpart, ycells)
    coeffs = jnp.stack((diffusion, drift))
    coef_wide = padded(coeffs, (("tm", 1), ("space", 3)), SWEEPS)

    def advance(current, forcing_now):
        source = current + forcing_now
        field = current
        widened = padded(jnp.stack((field, source)), (("tm", 1), ("space", 3)), SWEEPS)
        field = sweep_block(widened, coef_wide, SWEEPS)
        return (field, field)

    _, result = lax.scan(advance, initial, slabs)
    result = result.reshape(NT, zcells, xparts, xpart, ycells).transpose(0, 2, 1, 3, 4)
    result = result.reshape(NT * xparts, zcells, xpart, ycells)
    return lax.all_to_all(result, "tm", split_axis=0, concat_axis=1, tiled=True)


def gray(i):
    return i ^ (i >> 1)


def call(kernel, out_shape, operands, flags, scratch=(), flops=0, part=None):
    specs = [pl.BlockSpec(memory_space=pltpu.VMEM)] * len(operands)
    grid = ()
    if part:
        which, at, shape = part
        grid = (1,)
        specs[which] = pl.BlockSpec(shape, lambda _: (at,) + (0,) * (len(shape) - 1))
    size = sum(x.size * x.dtype.itemsize for x in operands)
    shapes = out_shape if isinstance(out_shape, (tuple, list)) else (out_shape,)
    size += sum(functools.reduce(lambda a, b: a * b, x.shape) * 4 for x in shapes)
    return pl.pallas_call(
        kernel,
        grid=grid,
        out_shape=out_shape,
        in_specs=[pl.BlockSpec(memory_space=pltpu.SMEM)] + specs,
        out_specs=jax.tree.map(lambda _: pl.BlockSpec(memory_space=pltpu.VMEM), out_shape),
        scratch_shapes=list(scratch),
        cost_estimate=pl.CostEstimate(flops=flops or size, bytes_accessed=size, transcendentals=0),
    )(flags, *operands)


def left_lanes():
    return lax.broadcasted_iota(jnp.int32, (ROWS, LANES), 1) < LANES // 2


def swap_lanes(v):
    return pltpu.roll(v, LANES // 2, 1)


def unrolled(count, one):
    depth = math.gcd(count, 4)

    def step(k, carry):
        for j in range(depth):
            one(depth * k + j)
        return carry

    lax.fori_loop(0, count // depth, step, 0)


def format_kernel(blocks, flags, raw, whole, send):
    zrows = raw.shape[0]
    left = left_lanes()

    def body(core):
        def one(pair):
            both = raw[pl.ds(2 * pair, 2)].reshape(LANES, LANES).T
            for r in range(blocks):
                low = both[2 * ROWS * r : 2 * ROWS * r + ROWS]
                high = both[2 * ROWS * r + ROWS : 2 * ROWS * (r + 1)]
                first = jnp.where(left, low, swap_lanes(high))
                second = jnp.where(left, swap_lanes(low), high)
                slot = gray(core * (blocks // 2) + r // 2)
                mine = gray(r) & 1 == core
                to = whole if mine else send
                start = (slot if mine else slot % (blocks // 2)) * ROWS * zrows + 2 * pair
                to[pl.ds(start, ROWS, stride=zrows), :] = first
                to[pl.ds(start + 1, ROWS, stride=zrows), :] = second

        unrolled(zrows // 2, one)

    for core in range(2):
        pl.when(flags[1] == core)(functools.partial(body, core))


def unformat_kernel(blocks, flags, whole, got, out):
    zrows = out.shape[0]
    left = left_lanes()

    def body(core):
        def one(pair):
            columns = []
            for r in range(blocks):
                slot = gray(core * (blocks // 2) + r // 2)
                mine = gray(r) & 1 == core
                src = whole if mine else got
                start = (slot if mine else slot % (blocks // 2)) * ROWS * zrows + 2 * pair
                first = src[pl.ds(start, ROWS, stride=zrows), :]
                second = src[pl.ds(start + 1, ROWS, stride=zrows), :]
                columns.append(jnp.where(left, first, swap_lanes(second)))
                columns.append(jnp.where(left, swap_lanes(first), second))
            both = jnp.concatenate(columns, axis=0).T
            out[pl.ds(2 * pair, 2)] = both.reshape(2, LANES // 2, LANES)

        unrolled(zrows // 2, one)

    for core in range(2):
        pl.when(flags[1] == core)(functools.partial(body, core))


def arrange_kernel(zpart, flags, got, out):
    chips, arrays = got.shape[0], out.shape[0]
    for k in range(arrays):
        for chip in range(chips):
            for upper in range(2):
                rows = pl.ds((2 * k + upper) * zpart, zpart)
                z = (upper * chips + chip) * zpart
                out[k, :, pl.ds(z, zpart), :] = got[chip, :, rows, :]


class Region:
    def __init__(self, even):
        self.even = even
        left = left_lanes()[None]
        self.left = left
        self.other = jnp.logical_xor(left, jnp.full((1, ROWS, LANES), even, jnp.int32) == 1)

    def tiles(self, plane):
        return plane.reshape(-1, ROWS, LANES)

    def plane(self, kind, m, own, core, link):
        back = ROWS - 1 - m
        if kind == "own":
            v = jnp.where(self.left, self.tiles(own[m]), self.tiles(own[back]))
        elif kind == "far":
            c = self.tiles(core[jnp.where(self.even == 1, back, m)])
            n = self.tiles(link[jnp.where(self.even == 1, m, back)])
            v = jnp.where(self.other, c, n)
        else:
            c = self.tiles(core[jnp.where(self.even == 1, m, back)])
            n = self.tiles(link[jnp.where(self.even == 1, back, m)])
            v = pltpu.roll(jnp.where(self.other, n, c), LANES // 2, 2)
        return v.reshape(-1, LANES)

    def fill(self, skip, own, core, link, put):
        def run(kind, start, stop, place):
            def step(k, carry):
                for j in range(FILL):
                    m = FILL * k + j
                    put(place(m), self.plane(kind, m, own, core, link))
                return carry

            lax.fori_loop(start, stop, step, 0)

        groups = ROWS // FILL
        run("own", 0, groups, lambda m: 2 * ROWS + m)
        run("near", 0, jnp.minimum(groups, 2 * groups - skip), lambda m: 2 * ROWS - 1 - m)
        run("far", jnp.minimum(skip, groups), groups, lambda m: m)


def prep_kernel(flags, own, core, link, coef):
    region = Region(flags[0])

    def put_diffusion(i, d):
        coef[0, i] = d

    def put_drift(i, r):
        d = coef[0, i]
        inv = 1.0 / (1.0 + 6.0 * d + r)
        coef[0, i] = d * inv
        coef[1, i] = (d + r) * inv
        coef[2, i] = inv

    region.fill(0, own.at[1], core.at[1], link.at[1], put_diffusion)
    region.fill(0, own.at[2], core.at[2], link.at[2], put_drift)


def window_kernel(done, flags, own, core, link, f_own, f_core, f_link, coef, *rest):
    if done:
        earlier, out, last, va, vb, c = rest
        out[0:done] = earlier[...]
    else:
        out, last, va, vb, c = rest
    steps, planes, zrows = f_core.shape[0], 3 * ROWS, own.shape[2]
    region = Region(flags[0])
    lane = lax.broadcasted_iota(jnp.int32, (ROWS, LANES), 1) % (LANES // 2)
    first_x, last_x = lane == 0, lane == LANES // 2 - 1
    inside = pl.ds(ROWS, zrows)
    ghost = planes + 1
    edge = jnp.zeros((planes + 2, ROWS, LANES), jnp.float32)
    for v in (va, vb):
        v[:, 0:ROWS] = edge
        v[:, zrows + ROWS :] = edge
        v[0, inside] = jnp.zeros((zrows, LANES), jnp.float32)

    def put_field(i, plane):
        va[1 + i, inside] = plane

    region.fill(0, own.at[0], core.at[0], link.at[0], put_field)
    va[ghost, inside] = swap_lanes(va[planes, inside])

    def relax(src, dst, first):
        cells = [(z, i) for z in range(0, zrows, ROWS) for i in reversed(range(first, planes))]
        for lead in range(0, len(cells), BATCH):
            part = cells[lead : lead + BATCH]
            field = [src[1 + i, ROWS + z : 2 * ROWS + z] for z, i in part]
            below = [pltpu.roll(v, 1, 1) for v in field]
            above = [pltpu.roll(v, LANES - 1, 1) for v in field]
            for (z, i), low, high in zip(part, below, above):
                at, rows = ROWS + z, slice(z, z + ROWS)
                zm = src[1 + i, at - 1 : at + ROWS - 1]
                total = src[1 + i, at + 1 : at + ROWS + 1]
                total += src[i, at : at + ROWS] + src[2 + i, at : at + ROWS]
                total += jnp.where(first_x, 0.0, low) + jnp.where(last_x, 0.0, high)
                new = c[i, rows] + coef[0, i, rows] * total + coef[1, i, rows] * zm
                dst[1 + i, at : at + ROWS] = new
        dst[ghost, inside] = swap_lanes(dst[planes, inside])

    def advance(first, step, carry):
        def put_source(i, plane):
            c[i] = coef[2, i] * (va[1 + i, inside] + plane)

        region.fill(SWEEPS * step // FILL, f_own.at[step], f_core.at[step], f_link.at[step], put_source)

        def pair(n, carry):
            relax(va, vb, first)
            relax(vb, va, first)
            return carry

        lax.fori_loop(0, SWEEPS // 2, pair, 0)
        for m in range(ROWS):
            low = region.tiles(va[1 + 2 * ROWS + m, inside])
            high = region.tiles(va[planes - m, inside])
            out[done + step, m] = jnp.where(region.left, low, high).reshape(-1, LANES)
        return carry

    half = steps // 2
    lax.fori_loop(0, half, functools.partial(advance, 1), 0)
    lax.fori_loop(half, steps, functools.partial(advance, SWEEPS * half + 1), 0)
    last[0] = out[done + steps - 1]


def split_along_y(forcing, initial, diffusion, drift):
    f32 = jnp.float32
    chips = lax.axis_size("tm") // 2
    zpart, xlen, ylen = initial.shape
    zlen = forcing.shape[1]
    blocks = ylen // (2 * ROWS)
    spw = 2 * ROWS // SWEEPS
    t, s = lax.axis_index("tm"), lax.axis_index("space")
    device = 2 * (t % chips) + s
    odd = device
    for shift in (1, 2, 4, 8):
        odd = odd ^ (odd >> shift)
    lower = t < chips
    flags = jnp.stack([1 - (odd & 1), s, jnp.int32(0)]).astype(jnp.int32)
    groups = [list(range(chips)), list(range(chips, 2 * chips))]
    both = ("tm", "space")
    across = []
    for b in range(1, 2 * chips - 1, 2):
        for base in (0, 2 * chips):
            i, j = base + gray(b), base + gray(b + 1)
            across += [(i, j), (j, i)]
    hop = [(i, 2 * chips + i) for i in range(2 * chips)]
    cores = [(0, 1), (1, 0)]

    def exchange(x):
        return lax.ppermute(x, "space", cores), lax.ppermute(x, both, across)

    def packed(raw):
        zr = raw.shape[0]
        shapes = [jax.ShapeDtypeStruct((n * ROWS * zr, LANES), f32) for n in (blocks, blocks // 2)]
        whole, send = call(functools.partial(format_kernel, blocks), shapes, (raw,), flags)
        got = lax.ppermute(send, "space", cores)
        whole = lax.dynamic_update_slice_in_dim(whole, got, (1 - s) * got.shape[0], 0)
        return whole.reshape(chips, ROWS, zr, LANES)

    def to_chips(x):
        return lax.all_to_all(x, "tm", 0, 0, axis_index_groups=groups, tiled=True)

    fields = jnp.stack((initial, diffusion, drift))
    far = lax.ppermute(fields, "tm", [(i, (i + chips) % (2 * chips)) for i in range(2 * chips)])
    force = packed(forcing.reshape(zlen, xlen, ylen))
    low, high = jnp.where(lower, fields, far), jnp.where(lower, far, fields)
    fields = jnp.concatenate([low[:, None], high[:, None]], axis=1).reshape(-1, xlen, ylen)
    force = to_chips(force)
    fields, force = lax.optimization_barrier((packed(fields), force))
    fields = to_chips(fields)
    fields = call(
        functools.partial(arrange_kernel, zpart),
        jax.ShapeDtypeStruct((3, ROWS, zlen, LANES), f32),
        (fields,),
        flags,
    )
    near = exchange(fields)
    region = jax.ShapeDtypeStruct((3, 3 * ROWS, zlen, LANES), f32)
    coef = call(prep_kernel, region, (fields, *near), flags)
    halos = [exchange(force[k : k + spw]) for k in range(0, chips, spw)]

    wide = pltpu.VMEM((3 * ROWS + 2, zlen + 2 * ROWS, LANES), f32)
    scratch = (
        wide,
        wide,
        pltpu.VMEM((3 * ROWS, zlen, LANES), f32),
    )
    flops = 10 * spw * SWEEPS * 2 * ROWS * zlen * LANES
    block = jax.ShapeDtypeStruct((1, ROWS, zlen, LANES), f32)

    def window(state, beside, k, earlier):
        done = k * spw
        return call(
            functools.partial(window_kernel, done),
            (jax.ShapeDtypeStruct((done + spw, ROWS, zlen, LANES), f32), block),
            (state, *beside, force, *halos[k], coef, *earlier),
            flags,
            scratch,
            flops,
            part=(3, k, (spw, ROWS, zlen, LANES)),
        )

    state, beside = fields, near
    for stage in range(2):
        earlier = ()
        for k in range(len(halos)):
            if k or stage:
                beside = exchange(state)
            result, state = window(state, beside, k, earlier)
            earlier = (result,)
        if stage == 0:
            state = jnp.where(lower, fields[0:1], lax.ppermute(state, both, hop))

    result = to_chips(result)
    send = lax.dynamic_slice_in_dim(result, (1 - s) * (chips // 2), chips // 2)
    got = lax.ppermute(send, "space", cores)
    out = call(
        functools.partial(unformat_kernel, blocks),
        jax.ShapeDtypeStruct((zlen, xlen, ylen), f32),
        (result.reshape(-1, LANES), got.reshape(-1, LANES)),
        flags,
    )
    return out[None]


def per_device(forcing, initial, diffusion, drift):
    tm, space = lax.axis_size("tm"), lax.axis_size("space")
    zpart, xlen, ylen = initial.shape
    chips, spw = tm // 2, 2 * ROWS // SWEEPS
    along_y = (
        tm == NT
        and space == 2
        and forcing.shape == (1, tm * zpart, xlen, ylen)
        and 2 * xlen == LANES
        and ylen == LANES
        and ylen * space == 2 * ROWS * 2 * chips
        and chips % spw == 0
        and chips * zpart % ROWS == 0
    )
    plan = split_along_y if along_y else split_along_z
    return plan(forcing, initial, diffusion, drift)


def solution(mesh):
    in_specs = (
        P("tm", None, None, "space"),
        P("tm", None, "space"),
        P("tm", None, "space"),
        P("tm", None, "space"),
    )
    out_specs = P("tm", None, None, "space")
    return jax.shard_map(
        per_device, mesh=mesh, in_specs=in_specs, out_specs=out_specs, check_vma=False
    )
```

```python
import functools
import math

import jax
import jax.numpy as jnp
from jax import lax
from jax.experimental import pallas as pl
from jax.experimental.pallas import tpu as pltpu
from jax.sharding import PartitionSpec as P


NT = 16
SWEEPS = 4
LANES = 128
ROWS = 8
FILL = 4
BATCH = 24
VMEM = 24 << 20


def padded(shard, sides, width):
    for axis, dim in sides:
        size, length = (lax.axis_size(axis), shard.shape[dim])
        up = [(i, (i + 1) % size) for i in range(size - 1)]
        down = [(j, i) for i, j in up]
        last = lax.slice_in_dim(shard, length - width, length, axis=dim)
        leading = lax.slice_in_dim(shard, 0, width, axis=dim)
        before = lax.ppermute(last, axis, up)
        after = lax.ppermute(leading, axis, down)
        shard = jnp.concatenate([before, shard, after], axis=dim)
    return shard


def relax_cells(field, source, diffus, drift_rate):
    widened = jnp.pad(field, ((0, 0), (1, 1), (0, 0)))
    beside = field[2:, :, 1:-1] + field[:-2, :, 1:-1]
    beside = beside + field[1:-1, :, 2:] + field[1:-1, :, :-2]
    beside = beside + widened[1:-1, 2:, 1:-1] + widened[1:-1, :-2, 1:-1]
    upstream = field[:-2, :, 1:-1]
    return (source + diffus * beside + drift_rate * upstream) / (1.0 + 6.0 * diffus + drift_rate)


def trim_rim(values, margin_cut):
    zlen = values.shape[-3]
    ylen = values.shape[-1]
    return values[..., margin_cut : zlen - margin_cut, :, margin_cut : ylen - margin_cut]


def sweep_block(widened, coef_wide, depth):
    grown = widened[0]
    for inner in range(depth):
        margin_cut = inner + 1
        grown = relax_cells(
            grown,
            trim_rim(widened[1], margin_cut),
            trim_rim(coef_wide[0], margin_cut),
            trim_rim(coef_wide[1], margin_cut),
        )
    return grown


def split_along_z(forcing, initial, diffusion, drift):
    xparts = lax.axis_size("tm") // NT
    slabs = lax.all_to_all(forcing, "tm", split_axis=1, concat_axis=0, tiled=True)
    zcells = slabs.shape[1]
    xpart = slabs.shape[2]
    ycells = slabs.shape[3]
    slabs = slabs.reshape(NT, xparts, zcells, xpart, ycells).transpose(0, 2, 1, 3, 4)
    slabs = slabs.reshape(NT, zcells, xparts * xpart, ycells)
    coeffs = jnp.stack((diffusion, drift))
    coef_wide = padded(coeffs, (("tm", 1), ("space", 3)), SWEEPS)

    def advance(current, forcing_now):
        source = current + forcing_now
        field = current
        widened = padded(jnp.stack((field, source)), (("tm", 1), ("space", 3)), SWEEPS)
        field = sweep_block(widened, coef_wide, SWEEPS)
        return (field, field)

    _, result = lax.scan(advance, initial, slabs)
    result = result.reshape(NT, zcells, xparts, xpart, ycells).transpose(0, 2, 1, 3, 4)
    result = result.reshape(NT * xparts, zcells, xpart, ycells)
    return lax.all_to_all(result, "tm", split_axis=0, concat_axis=1, tiled=True)


def gray(i):
    return i ^ (i >> 1)


def call(kernel, out_shape, operands, flags, scratch=(), flops=0, part=None):
    specs = [pl.BlockSpec(memory_space=pltpu.VMEM)] * len(operands)
    grid = ()
    if part:
        which, at, shape = part
        grid = (1,)
        specs[which] = pl.BlockSpec(shape, lambda _: (at,) + (0,) * (len(shape) - 1))
    size = sum(x.size * x.dtype.itemsize for x in operands)
    shapes = out_shape if isinstance(out_shape, (tuple, list)) else (out_shape,)
    size += sum(functools.reduce(lambda a, b: a * b, x.shape) * 4 for x in shapes)
    return pl.pallas_call(
        kernel,
        grid=grid,
        out_shape=out_shape,
        in_specs=[pl.BlockSpec(memory_space=pltpu.SMEM)] + specs,
        out_specs=jax.tree.map(lambda _: pl.BlockSpec(memory_space=pltpu.VMEM), out_shape),
        scratch_shapes=list(scratch),
        cost_estimate=pl.CostEstimate(flops=flops or size, bytes_accessed=size, transcendentals=0),
        compiler_params=pltpu.CompilerParams(vmem_limit_bytes=VMEM),
    )(flags, *operands)


def left_lanes():
    return lax.broadcasted_iota(jnp.int32, (ROWS, LANES), 1) < LANES // 2


def swap_lanes(v):
    return pltpu.roll(v, LANES // 2, 1)


def unrolled(count, one):
    depth = math.gcd(count, 4)

    def step(k, carry):
        for j in range(depth):
            one(depth * k + j)
        return carry

    lax.fori_loop(0, count // depth, step, 0)


def format_kernel(blocks, flags, raw, whole, send):
    zrows = raw.shape[0]
    left = left_lanes()

    def body(core):
        def one(pair):
            both = raw[pl.ds(2 * pair, 2)].reshape(LANES, LANES).T
            for r in range(blocks):
                low = both[2 * ROWS * r : 2 * ROWS * r + ROWS]
                high = both[2 * ROWS * r + ROWS : 2 * ROWS * (r + 1)]
                first = jnp.where(left, low, swap_lanes(high))
                second = jnp.where(left, swap_lanes(low), high)
                slot = gray(core * (blocks // 2) + r // 2)
                mine = gray(r) & 1 == core
                to = whole if mine else send
                start = (slot if mine else slot % (blocks // 2)) * ROWS * zrows + 2 * pair
                to[pl.ds(start, ROWS, stride=zrows), :] = first
                to[pl.ds(start + 1, ROWS, stride=zrows), :] = second

        unrolled(zrows // 2, one)

    for core in range(2):
        pl.when(flags[1] == core)(functools.partial(body, core))


def unformat_kernel(blocks, flags, whole, got, out):
    zrows = out.shape[0]
    left = left_lanes()

    def body(core):
        def one(pair):
            columns = []
            for r in range(blocks):
                slot = gray(core * (blocks // 2) + r // 2)
                mine = gray(r) & 1 == core
                src = whole if mine else got
                start = (slot if mine else slot % (blocks // 2)) * ROWS * zrows + 2 * pair
                first = src[pl.ds(start, ROWS, stride=zrows), :]
                second = src[pl.ds(start + 1, ROWS, stride=zrows), :]
                columns.append(jnp.where(left, first, swap_lanes(second)))
                columns.append(jnp.where(left, swap_lanes(first), second))
            both = jnp.concatenate(columns, axis=0).T
            out[pl.ds(2 * pair, 2)] = both.reshape(2, LANES // 2, LANES)

        unrolled(zrows // 2, one)

    for core in range(2):
        pl.when(flags[1] == core)(functools.partial(body, core))


def arrange_kernel(zpart, flags, got, out):
    chips, arrays = got.shape[0], out.shape[0]
    for k in range(arrays):
        for chip in range(chips):
            for upper in range(2):
                rows = pl.ds((2 * k + upper) * zpart, zpart)
                z = (upper * chips + chip) * zpart
                out[k, :, pl.ds(z, zpart), :] = got[chip, :, rows, :]


class Region:
    def __init__(self, even):
        self.even = even
        left = left_lanes()[None]
        self.left = left
        self.other = jnp.logical_xor(left, jnp.full((1, ROWS, LANES), even, jnp.int32) == 1)

    def tiles(self, plane):
        return plane.reshape(-1, ROWS, LANES)

    def plane(self, kind, m, own, core, link):
        back = ROWS - 1 - m
        if kind == "own":
            v = jnp.where(self.left, self.tiles(own[m]), self.tiles(own[back]))
        elif kind == "far":
            c = self.tiles(core[jnp.where(self.even == 1, back, m)])
            n = self.tiles(link[jnp.where(self.even == 1, m, back)])
            v = jnp.where(self.other, c, n)
        else:
            c = self.tiles(core[jnp.where(self.even == 1, m, back)])
            n = self.tiles(link[jnp.where(self.even == 1, back, m)])
            v = pltpu.roll(jnp.where(self.other, n, c), LANES // 2, 2)
        return v.reshape(-1, LANES)

    def fill(self, skip, own, core, link, put):
        def run(kind, start, stop, place):
            def step(k, carry):
                for j in range(FILL):
                    m = FILL * k + j
                    put(place(m), self.plane(kind, m, own, core, link))
                return carry

            lax.fori_loop(start, stop, step, 0)

        groups = ROWS // FILL
        run("own", 0, groups, lambda m: 2 * ROWS + m)
        run("near", 0, jnp.minimum(groups, 2 * groups - skip), lambda m: 2 * ROWS - 1 - m)
        run("far", jnp.minimum(skip, groups), groups, lambda m: m)


def prep_kernel(flags, own, core, link, coef):
    region = Region(flags[0])

    def put_diffusion(i, d):
        coef[0, i] = d

    def put_drift(i, r):
        d = coef[0, i]
        inv = 1.0 / (1.0 + 6.0 * d + r)
        coef[0, i] = d * inv
        coef[1, i] = (d + r) * inv
        coef[2, i] = inv

    region.fill(0, own.at[1], core.at[1], link.at[1], put_diffusion)
    region.fill(0, own.at[2], core.at[2], link.at[2], put_drift)


def window_kernel(done, flags, own, core, link, f_own, f_core, f_link, coef, *rest):
    if done:
        earlier, out, last, va, vb, c = rest
        out[0:done] = earlier[...]
    else:
        out, last, va, vb, c = rest
    steps, planes, zrows = f_core.shape[0], 3 * ROWS, own.shape[2]
    region = Region(flags[0])
    lane = lax.broadcasted_iota(jnp.int32, (ROWS, LANES), 1) % (LANES // 2)
    first_x, last_x = lane == 0, lane == LANES // 2 - 1
    inside = pl.ds(ROWS, zrows)
    ghost = planes + 1
    edge = jnp.zeros((planes + 2, ROWS, LANES), jnp.float32)
    for v in (va, vb):
        v[:, 0:ROWS] = edge
        v[:, zrows + ROWS :] = edge
        v[0, inside] = jnp.zeros((zrows, LANES), jnp.float32)

    def put_field(i, plane):
        va[1 + i, inside] = plane

    region.fill(0, own.at[0], core.at[0], link.at[0], put_field)
    va[ghost, inside] = swap_lanes(va[planes, inside])

    def relax(src, dst, first):
        cells = [(z, i) for i in reversed(range(first, planes)) for z in range(0, zrows, ROWS)]
        for lead in range(0, len(cells), BATCH):
            part = cells[lead : lead + BATCH]
            field = [src[1 + i, ROWS + z : 2 * ROWS + z] for z, i in part]
            below = [pltpu.roll(v, 1, 1) for v in field]
            above = [pltpu.roll(v, LANES - 1, 1) for v in field]
            for (z, i), low, high in zip(part, below, above):
                at, rows = ROWS + z, slice(z, z + ROWS)
                zm = src[1 + i, at - 1 : at + ROWS - 1]
                total = src[1 + i, at + 1 : at + ROWS + 1]
                total += src[i, at : at + ROWS] + src[2 + i, at : at + ROWS]
                total += jnp.where(first_x, 0.0, low) + jnp.where(last_x, 0.0, high)
                new = c[i, rows] + coef[0, i, rows] * total + coef[1, i, rows] * zm
                dst[1 + i, at : at + ROWS] = new
        dst[ghost, inside] = swap_lanes(dst[planes, inside])

    def advance(first, step, carry):
        def put_source(i, plane):
            c[i] = coef[2, i] * (va[1 + i, inside] + plane)

        region.fill(SWEEPS * step // FILL, f_own.at[step], f_core.at[step], f_link.at[step], put_source)

        def pair(n, carry):
            relax(va, vb, first)
            relax(vb, va, first)
            return carry

        lax.fori_loop(0, SWEEPS // 2, pair, 0)
        for m in range(ROWS):
            low = region.tiles(va[1 + 2 * ROWS + m, inside])
            high = region.tiles(va[planes - m, inside])
            out[done + step, m] = jnp.where(region.left, low, high).reshape(-1, LANES)
        return carry

    half = steps // 2
    lax.fori_loop(0, half, functools.partial(advance, 1), 0)
    lax.fori_loop(half, steps, functools.partial(advance, SWEEPS * half + 1), 0)
    last[0] = out[done + steps - 1]


def split_along_y(forcing, initial, diffusion, drift):
    f32 = jnp.float32
    chips = lax.axis_size("tm") // 2
    zpart, xlen, ylen = initial.shape
    zlen = forcing.shape[1]
    blocks = ylen // (2 * ROWS)
    spw = 2 * ROWS // SWEEPS
    t, s = lax.axis_index("tm"), lax.axis_index("space")
    device = 2 * (t % chips) + s
    odd = device
    for shift in (1, 2, 4, 8):
        odd = odd ^ (odd >> shift)
    lower = t < chips
    flags = jnp.stack([1 - (odd & 1), s, jnp.int32(0)]).astype(jnp.int32)
    groups = [list(range(chips)), list(range(chips, 2 * chips))]
    both = ("tm", "space")
    across = []
    for b in range(1, 2 * chips - 1, 2):
        for base in (0, 2 * chips):
            i, j = base + gray(b), base + gray(b + 1)
            across += [(i, j), (j, i)]
    hop = [(i, 2 * chips + i) for i in range(2 * chips)]
    cores = [(0, 1), (1, 0)]

    def exchange(x):
        return lax.ppermute(x, "space", cores), lax.ppermute(x, both, across)

    def packed(raw):
        zr = raw.shape[0]
        shapes = [jax.ShapeDtypeStruct((n * ROWS * zr, LANES), f32) for n in (blocks, blocks // 2)]
        whole, send = call(functools.partial(format_kernel, blocks), shapes, (raw,), flags)
        got = lax.ppermute(send, "space", cores)
        whole = lax.dynamic_update_slice_in_dim(whole, got, (1 - s) * got.shape[0], 0)
        return whole.reshape(chips, ROWS, zr, LANES)

    def to_chips(x):
        return lax.all_to_all(x, "tm", 0, 0, axis_index_groups=groups, tiled=True)

    fields = jnp.stack((initial, diffusion, drift))
    far = lax.ppermute(fields, "tm", [(i, (i + chips) % (2 * chips)) for i in range(2 * chips)])
    force = packed(forcing.reshape(zlen, xlen, ylen))
    low, high = jnp.where(lower, fields, far), jnp.where(lower, far, fields)
    fields = jnp.concatenate([low[:, None], high[:, None]], axis=1).reshape(-1, xlen, ylen)
    force = to_chips(force)
    fields, force = lax.optimization_barrier((packed(fields), force))
    fields = to_chips(fields)
    fields = call(
        functools.partial(arrange_kernel, zpart),
        jax.ShapeDtypeStruct((3, ROWS, zlen, LANES), f32),
        (fields,),
        flags,
    )
    near = exchange(fields)
    region = jax.ShapeDtypeStruct((3, 3 * ROWS, zlen, LANES), f32)
    coef = call(prep_kernel, region, (fields, *near), flags)
    halos = []
    for k in range(0, chips, spw):
        halos.append(exchange(force[k : k + spw]))

    wide = pltpu.VMEM((3 * ROWS + 2, zlen + 2 * ROWS, LANES), f32)
    scratch = (
        wide,
        wide,
        pltpu.VMEM((3 * ROWS, zlen, LANES), f32),
    )
    flops = 10 * spw * SWEEPS * 2 * ROWS * zlen * LANES
    block = jax.ShapeDtypeStruct((1, ROWS, zlen, LANES), f32)

    def window(state, beside, k, earlier):
        done = k * spw
        return call(
            functools.partial(window_kernel, done),
            (jax.ShapeDtypeStruct((done + spw, ROWS, zlen, LANES), f32), block),
            (state, *beside, force, *halos[k], coef, *earlier),
            flags,
            scratch,
            flops,
            part=(3, k, (spw, ROWS, zlen, LANES)),
        )

    state, beside = fields, near
    for stage in range(2):
        earlier = ()
        for k in range(len(halos)):
            if k or stage:
                beside = exchange(state)
            result, state = window(state, beside, k, earlier)
            earlier = (result,)
        if stage == 0:
            state = jnp.where(lower, fields[0:1], lax.ppermute(state, both, hop))

    result = to_chips(result)
    send = lax.dynamic_slice_in_dim(result, (1 - s) * (chips // 2), chips // 2)
    got = lax.ppermute(send, "space", cores)
    out = call(
        functools.partial(unformat_kernel, blocks),
        jax.ShapeDtypeStruct((zlen, xlen, ylen), f32),
        (result.reshape(-1, LANES), got.reshape(-1, LANES)),
        flags,
    )
    return out[None]


def per_device(forcing, initial, diffusion, drift):
    tm, space = lax.axis_size("tm"), lax.axis_size("space")
    zpart, xlen, ylen = initial.shape
    chips, spw = tm // 2, 2 * ROWS // SWEEPS
    along_y = (
        tm == NT
        and space == 2
        and forcing.shape == (1, tm * zpart, xlen, ylen)
        and 2 * xlen == LANES
        and ylen == LANES
        and ylen * space == 2 * ROWS * 2 * chips
        and chips % spw == 0
        and chips * zpart % ROWS == 0
    )
    plan = split_along_y if along_y else split_along_z
    return plan(forcing, initial, diffusion, drift)


def solution(mesh):
    in_specs = (
        P("tm", None, None, "space"),
        P("tm", None, "space"),
        P("tm", None, "space"),
        P("tm", None, "space"),
    )
    out_specs = P("tm", None, None, "space")
    return jax.shard_map(
        per_device, mesh=mesh, in_specs=in_specs, out_specs=out_specs, check_vma=False
    )
```

```python
import functools
import math

import jax
import jax.numpy as jnp
from jax import lax
from jax.experimental import pallas as pl
from jax.experimental.pallas import tpu as pltpu
from jax.sharding import PartitionSpec as P


NT = 16
SWEEPS = 4
LANES = 128
ROWS = 8
FILL = 4
BATCH = 16
VMEM = 24 << 20


def padded(shard, sides, width):
    for axis, dim in sides:
        size, length = (lax.axis_size(axis), shard.shape[dim])
        up = [(i, (i + 1) % size) for i in range(size - 1)]
        down = [(j, i) for i, j in up]
        last = lax.slice_in_dim(shard, length - width, length, axis=dim)
        leading = lax.slice_in_dim(shard, 0, width, axis=dim)
        before = lax.ppermute(last, axis, up)
        after = lax.ppermute(leading, axis, down)
        shard = jnp.concatenate([before, shard, after], axis=dim)
    return shard


def relax_cells(field, source, diffus, drift_rate):
    widened = jnp.pad(field, ((0, 0), (1, 1), (0, 0)))
    beside = field[2:, :, 1:-1] + field[:-2, :, 1:-1]
    beside = beside + field[1:-1, :, 2:] + field[1:-1, :, :-2]
    beside = beside + widened[1:-1, 2:, 1:-1] + widened[1:-1, :-2, 1:-1]
    upstream = field[:-2, :, 1:-1]
    return (source + diffus * beside + drift_rate * upstream) / (1.0 + 6.0 * diffus + drift_rate)


def trim_rim(values, margin_cut):
    zlen = values.shape[-3]
    ylen = values.shape[-1]
    return values[..., margin_cut : zlen - margin_cut, :, margin_cut : ylen - margin_cut]


def sweep_block(widened, coef_wide, depth):
    grown = widened[0]
    for inner in range(depth):
        margin_cut = inner + 1
        grown = relax_cells(
            grown,
            trim_rim(widened[1], margin_cut),
            trim_rim(coef_wide[0], margin_cut),
            trim_rim(coef_wide[1], margin_cut),
        )
    return grown


def split_along_z(forcing, initial, diffusion, drift):
    xparts = lax.axis_size("tm") // NT
    slabs = lax.all_to_all(forcing, "tm", split_axis=1, concat_axis=0, tiled=True)
    zcells = slabs.shape[1]
    xpart = slabs.shape[2]
    ycells = slabs.shape[3]
    slabs = slabs.reshape(NT, xparts, zcells, xpart, ycells).transpose(0, 2, 1, 3, 4)
    slabs = slabs.reshape(NT, zcells, xparts * xpart, ycells)
    coeffs = jnp.stack((diffusion, drift))
    coef_wide = padded(coeffs, (("tm", 1), ("space", 3)), SWEEPS)

    def advance(current, forcing_now):
        source = current + forcing_now
        field = current
        widened = padded(jnp.stack((field, source)), (("tm", 1), ("space", 3)), SWEEPS)
        field = sweep_block(widened, coef_wide, SWEEPS)
        return (field, field)

    _, result = lax.scan(advance, initial, slabs)
    result = result.reshape(NT, zcells, xparts, xpart, ycells).transpose(0, 2, 1, 3, 4)
    result = result.reshape(NT * xparts, zcells, xpart, ycells)
    return lax.all_to_all(result, "tm", split_axis=0, concat_axis=1, tiled=True)


def gray(i):
    return i ^ (i >> 1)


def call(kernel, out_shape, operands, flags, scratch=(), flops=0, part=None, grant=VMEM):
    specs = [pl.BlockSpec(memory_space=pltpu.VMEM)] * len(operands)
    grid = ()
    if part:
        which, at, shape = part
        grid = (1,)
        specs[which] = pl.BlockSpec(shape, lambda _: (at,) + (0,) * (len(shape) - 1))
    size = sum(x.size * x.dtype.itemsize for x in operands)
    shapes = out_shape if isinstance(out_shape, (tuple, list)) else (out_shape,)
    size += sum(functools.reduce(lambda a, b: a * b, x.shape) * 4 for x in shapes)
    return pl.pallas_call(
        kernel,
        grid=grid,
        out_shape=out_shape,
        in_specs=[pl.BlockSpec(memory_space=pltpu.SMEM)] + specs,
        out_specs=jax.tree.map(lambda _: pl.BlockSpec(memory_space=pltpu.VMEM), out_shape),
        scratch_shapes=list(scratch),
        cost_estimate=pl.CostEstimate(flops=flops or size, bytes_accessed=size, transcendentals=0),
        compiler_params=pltpu.CompilerParams(vmem_limit_bytes=grant),
    )(flags, *operands)


def left_lanes():
    return lax.broadcasted_iota(jnp.int32, (ROWS, LANES), 1) < LANES // 2


def swap_lanes(v):
    return pltpu.roll(v, LANES // 2, 1)


def unrolled(count, one):
    depth = math.gcd(count, 8)

    def step(k, carry):
        for j in range(depth):
            one(depth * k + j)
        return carry

    lax.fori_loop(0, count // depth, step, 0)


def format_kernel(blocks, flags, raw, whole, send):
    zrows = raw.shape[0]
    left = left_lanes()

    def body(core):
        def one(pair):
            both = raw[pl.ds(2 * pair, 2)].reshape(LANES, LANES).T
            for r in range(blocks):
                low = both[2 * ROWS * r : 2 * ROWS * r + ROWS]
                high = both[2 * ROWS * r + ROWS : 2 * ROWS * (r + 1)]
                first = jnp.where(left, low, swap_lanes(high))
                second = jnp.where(left, swap_lanes(low), high)
                slot = gray(core * (blocks // 2) + r // 2)
                mine = gray(r) & 1 == core
                to = whole if mine else send
                start = (slot if mine else slot % (blocks // 2)) * ROWS * zrows + 2 * pair
                to[pl.ds(start, ROWS, stride=zrows), :] = first
                to[pl.ds(start + 1, ROWS, stride=zrows), :] = second

        unrolled(zrows // 2, one)

    for core in range(2):
        pl.when(flags[1] == core)(functools.partial(body, core))


def unformat_kernel(blocks, flags, whole, got, out):
    zrows = out.shape[0]
    left = left_lanes()

    def body(core):
        def one(pair):
            columns = []
            for r in range(blocks):
                slot = gray(core * (blocks // 2) + r // 2)
                mine = gray(r) & 1 == core
                src = whole if mine else got
                start = (slot if mine else slot % (blocks // 2)) * ROWS * zrows + 2 * pair
                first = src[pl.ds(start, ROWS, stride=zrows), :]
                second = src[pl.ds(start + 1, ROWS, stride=zrows), :]
                columns.append(jnp.where(left, first, swap_lanes(second)))
                columns.append(jnp.where(left, swap_lanes(first), second))
            both = jnp.concatenate(columns, axis=0).T
            out[pl.ds(2 * pair, 2)] = both.reshape(2, LANES // 2, LANES)

        unrolled(zrows // 2, one)

    for core in range(2):
        pl.when(flags[1] == core)(functools.partial(body, core))


def arrange_kernel(zpart, flags, got, out):
    chips, arrays = got.shape[0], out.shape[0]
    for k in range(arrays):
        for chip in range(chips):
            for upper in range(2):
                rows = pl.ds((2 * k + upper) * zpart, zpart)
                z = (upper * chips + chip) * zpart
                out[k, :, pl.ds(z, zpart), :] = got[chip, :, rows, :]


class Region:
    def __init__(self, even):
        self.even = even
        left = left_lanes()[None]
        self.left = left
        self.other = jnp.logical_xor(left, jnp.full((1, ROWS, LANES), even, jnp.int32) == 1)

    def tiles(self, plane):
        return plane.reshape(-1, ROWS, LANES)

    def plane(self, kind, m, own, core, link):
        back = ROWS - 1 - m
        if kind == "own":
            v = jnp.where(self.left, self.tiles(own[m]), self.tiles(own[back]))
        elif kind == "far":
            c = self.tiles(core[jnp.where(self.even == 1, back, m)])
            n = self.tiles(link[jnp.where(self.even == 1, m, back)])
            v = jnp.where(self.other, c, n)
        else:
            c = self.tiles(core[jnp.where(self.even == 1, m, back)])
            n = self.tiles(link[jnp.where(self.even == 1, back, m)])
            v = pltpu.roll(jnp.where(self.other, n, c), LANES // 2, 2)
        return v.reshape(-1, LANES)

    def fill(self, skip, own, core, link, put):
        def run(kind, start, stop, place):
            def step(k, carry):
                for j in range(FILL):
                    m = FILL * k + j
                    put(place(m), self.plane(kind, m, own, core, link))
                return carry

            lax.fori_loop(start, stop, step, 0)

        groups = ROWS // FILL
        run("own", 0, groups, lambda m: 2 * ROWS + m)
        run("near", 0, jnp.minimum(groups, 2 * groups - skip), lambda m: 2 * ROWS - 1 - m)
        run("far", jnp.minimum(skip, groups), groups, lambda m: m)


def prep_kernel(flags, own, core, link, coef):
    region = Region(flags[0])

    def put_diffusion(i, d):
        coef[0, i] = d

    def put_drift(i, r):
        d = coef[0, i]
        inv = 1.0 / (1.0 + 6.0 * d + r)
        coef[0, i] = d * inv
        coef[1, i] = (d + r) * inv
        coef[2, i] = inv

    region.fill(0, own.at[1], core.at[1], link.at[1], put_diffusion)
    region.fill(0, own.at[2], core.at[2], link.at[2], put_drift)


def window_kernel(done, flags, own, core, link, f_own, f_core, f_link, coef, *rest):
    if done:
        earlier, out, last, va, vb, c = rest
        out[0:done] = earlier[...]
    else:
        out, last, va, vb, c = rest
    steps, planes, zrows = f_core.shape[0], 3 * ROWS, own.shape[2]
    region = Region(flags[0])
    lane = lax.broadcasted_iota(jnp.int32, (ROWS, LANES), 1) % (LANES // 2)
    first_x, last_x = lane == 0, lane == LANES // 2 - 1
    inside = pl.ds(ROWS, zrows)
    ghost = planes + 1
    edge = jnp.zeros((planes + 2, ROWS, LANES), jnp.float32)
    for v in (va, vb):
        v[:, 0:ROWS] = edge
        v[:, zrows + ROWS :] = edge
        v[0, inside] = jnp.zeros((zrows, LANES), jnp.float32)

    def put_field(i, plane):
        va[1 + i, inside] = plane

    region.fill(0, own.at[0], core.at[0], link.at[0], put_field)
    va[ghost, inside] = swap_lanes(va[planes, inside])

    def relax(src, dst, first):
        cells = [(z, i) for i in reversed(range(first, planes)) for z in range(0, zrows, ROWS)]
        for lead in range(0, len(cells), BATCH):
            part = cells[lead : lead + BATCH]
            field = [src[1 + i, ROWS + z : 2 * ROWS + z] for z, i in part]
            below = [pltpu.roll(v, 1, 1) for v in field]
            above = [pltpu.roll(v, LANES - 1, 1) for v in field]
            for (z, i), low, high in zip(part, below, above):
                at, rows = ROWS + z, slice(z, z + ROWS)
                zm = src[1 + i, at - 1 : at + ROWS - 1]
                total = src[1 + i, at + 1 : at + ROWS + 1]
                total += src[i, at : at + ROWS] + src[2 + i, at : at + ROWS]
                total += jnp.where(first_x, 0.0, low) + jnp.where(last_x, 0.0, high)
                new = c[i, rows] + coef[0, i, rows] * total + coef[1, i, rows] * zm
                dst[1 + i, at : at + ROWS] = new
        dst[ghost, inside] = swap_lanes(dst[planes, inside])

    def advance(first, step):
        def put_source(i, plane):
            c[i] = coef[2, i] * (va[1 + i, inside] + plane)

        region.fill(SWEEPS * step // FILL, f_own.at[step], f_core.at[step], f_link.at[step], put_source)

        def pair(n, carry):
            relax(va, vb, first)
            relax(vb, va, first)
            return carry

        lax.fori_loop(0, SWEEPS // 2, pair, 0)
        for m in range(ROWS):
            low = region.tiles(va[1 + 2 * ROWS + m, inside])
            high = region.tiles(va[planes - m, inside])
            out[done + step, m] = jnp.where(region.left, low, high).reshape(-1, LANES)

    for step in range(steps):
        advance(SWEEPS * step + 1, step)
    last[0] = out[done + steps - 1]


def split_along_y(forcing, initial, diffusion, drift):
    f32 = jnp.float32
    chips = lax.axis_size("tm") // 2
    zpart, xlen, ylen = initial.shape
    zlen = forcing.shape[1]
    blocks = ylen // (2 * ROWS)
    spw = 2 * ROWS // SWEEPS
    t, s = lax.axis_index("tm"), lax.axis_index("space")
    device = 2 * (t % chips) + s
    odd = device
    for shift in (1, 2, 4, 8):
        odd = odd ^ (odd >> shift)
    lower = t < chips
    flags = jnp.stack([1 - (odd & 1), s, jnp.int32(0)]).astype(jnp.int32)
    groups = [list(range(chips)), list(range(chips, 2 * chips))]
    both = ("tm", "space")
    across = []
    for b in range(1, 2 * chips - 1, 2):
        for base in (0, 2 * chips):
            i, j = base + gray(b), base + gray(b + 1)
            across += [(i, j), (j, i)]
    hop = [(i, 2 * chips + i) for i in range(2 * chips)]
    cores = [(0, 1), (1, 0)]

    def exchange(x):
        return lax.ppermute(x, "space", cores), lax.ppermute(x, both, across)

    def packed(raw):
        zr = raw.shape[0]
        shapes = [jax.ShapeDtypeStruct((n * ROWS * zr, LANES), f32) for n in (blocks, blocks // 2)]
        whole, send = call(
            functools.partial(format_kernel, blocks),
            shapes,
            (raw,),
            flags,
            grant=None if zr == zlen else VMEM,
        )
        got = lax.ppermute(send, "space", cores)
        whole = lax.dynamic_update_slice_in_dim(whole, got, (1 - s) * got.shape[0], 0)
        return whole.reshape(chips, ROWS, zr, LANES)

    def to_chips(x):
        return lax.all_to_all(x, "tm", 0, 0, axis_index_groups=groups, tiled=True)

    fields = jnp.stack((initial, diffusion, drift))
    far = lax.ppermute(fields, "tm", [(i, (i + chips) % (2 * chips)) for i in range(2 * chips)])
    force = packed(forcing.reshape(zlen, xlen, ylen))
    low, high = jnp.where(lower, fields, far), jnp.where(lower, far, fields)
    fields = jnp.concatenate([low[:, None], high[:, None]], axis=1).reshape(-1, xlen, ylen)
    force = to_chips(force)
    fields, force = lax.optimization_barrier((packed(fields), force))
    fields = to_chips(fields)
    fields = call(
        functools.partial(arrange_kernel, zpart),
        jax.ShapeDtypeStruct((3, ROWS, zlen, LANES), f32),
        (fields,),
        flags,
    )
    near = exchange(fields)
    region = jax.ShapeDtypeStruct((3, 3 * ROWS, zlen, LANES), f32)
    coef = call(prep_kernel, region, (fields, *near), flags)
    halos = []
    for k in range(0, chips, spw):
        halos.append(exchange(force[k : k + spw]))

    wide = pltpu.VMEM((3 * ROWS + 2, zlen + 2 * ROWS, LANES), f32)
    scratch = (
        wide,
        wide,
        pltpu.VMEM((3 * ROWS, zlen, LANES), f32),
    )
    flops = 10 * spw * SWEEPS * 2 * ROWS * zlen * LANES
    block = jax.ShapeDtypeStruct((1, ROWS, zlen, LANES), f32)

    def window(state, beside, k, earlier):
        done = k * spw
        return call(
            functools.partial(window_kernel, done),
            (jax.ShapeDtypeStruct((done + spw, ROWS, zlen, LANES), f32), block),
            (state, *beside, force, *halos[k], coef, *earlier),
            flags,
            scratch,
            flops,
            part=(3, k, (spw, ROWS, zlen, LANES)),
        )

    state, beside = fields, near
    for stage in range(2):
        earlier = ()
        for k in range(len(halos)):
            if k or stage:
                beside = exchange(state)
            result, state = window(state, beside, k, earlier)
            earlier = (result,)
        if stage == 0:
            state = jnp.where(lower, fields[0:1], lax.ppermute(state, both, hop))

    result = to_chips(result)
    send = lax.dynamic_slice_in_dim(result, (1 - s) * (chips // 2), chips // 2)
    got = lax.ppermute(send, "space", cores)
    out = call(
        functools.partial(unformat_kernel, blocks),
        jax.ShapeDtypeStruct((zlen, xlen, ylen), f32),
        (result.reshape(-1, LANES), got.reshape(-1, LANES)),
        flags,
    )
    return out[None]


def per_device(forcing, initial, diffusion, drift):
    tm, space = lax.axis_size("tm"), lax.axis_size("space")
    zpart, xlen, ylen = initial.shape
    chips, spw = tm // 2, 2 * ROWS // SWEEPS
    along_y = (
        tm == NT
        and space == 2
        and forcing.shape == (1, tm * zpart, xlen, ylen)
        and 2 * xlen == LANES
        and ylen == LANES
        and ylen * space == 2 * ROWS * 2 * chips
        and chips % spw == 0
        and chips * zpart % ROWS == 0
    )
    plan = split_along_y if along_y else split_along_z
    return plan(forcing, initial, diffusion, drift)


def solution(mesh):
    in_specs = (
        P("tm", None, None, "space"),
        P("tm", None, "space"),
        P("tm", None, "space"),
        P("tm", None, "space"),
    )
    out_specs = P("tm", None, None, "space")
    return jax.shard_map(
        per_device, mesh=mesh, in_specs=in_specs, out_specs=out_specs, check_vma=False
    )
```
